32 devices in a mesh: seq: 8 (over z, y), samp: 4 (over x, core).
Axes of the slice: x: 2, y: 2, z: 4, core: 2. Of those that a mesh axis runs over, the one named last changes fastest.
Arguments:
- queries: bfloat16 [4, 1024, 5120], P('samp', 'seq'), may hold values from -120 to 120
- prefix_keys: bfloat16 [1024, 1024], P('seq'), may hold values from -4 to 4
- prefix_values: bfloat16 [1024, 1024], P('seq'), may hold values from -4 to 4
- suffix_keys: bfloat16 [4, 1024, 1024], P('samp', 'seq'), may hold values from -5 to 5
- suffix_values: bfloat16 [4, 1024, 1024], P('samp', 'seq'), may hold values from -4 to 4
- layout_pre: int32 [4, 8, 8], P('samp', 'seq'), may hold values 0 or 1
- layout_suf: int32 [4, 8, 8], P('samp', 'seq'), may hold values 0 or 1
- lengths: int32 [4], P('samp'), may hold values from 1 to 8
Outputs:
- attended: bfloat16 [4, 1024, 5120], P('samp', 'seq')
The draws below stay inside these ranges and needn't reach their ends.
All inputs are finite; a program needn't handle non-finite values. No bound on the sum of `layout_pre` or of `layout_suf` on one device may be relied on, other than what follows from the above.
Results may differ from the reference program's by a relative error of at most 0.004.
Values may be sent and summed in bfloat16 or wider, within the bound.
No kernel may reach another device: no remote copies, remote signals or barrier semaphores. Data moves between devices by JAX's collectives and lax.ppermute only.
A program may use at most 128 MiB of HBM per device.

```python
import math
import jax
import jax.numpy as jnp
from jax import lax

HEADS = 40
KV_HEADS = 8
HEAD_DIM = 128
BLOCK = 128
PREFIX = 1024
SUFFIX = 1024
SAMPLES = 4
PRE_BLOCKS = 8
SUF_BLOCKS = 8


def draw_pair(key):
    shape_keys = (SAMPLES, SUFFIX, KV_HEADS * HEAD_DIM)
    base_keys = jnp.clip(jax.random.normal(jax.random.fold_in(key, 11), shape_keys, jnp.float32), -4.0, 4.0)
    base_queries = 2.5 * jnp.clip(jax.random.normal(jax.random.fold_in(key, 12), (SAMPLES, SUFFIX, HEADS * HEAD_DIM), jnp.float32), -4.0, 4.0)
    return (base_queries, base_keys)


def draw_queries(key, part):
    return draw_pair(key)[0].astype(jnp.bfloat16)


def draw_suffix_keys(key, part):
    return draw_pair(key)[1].astype(jnp.bfloat16)


def plant(array, key, least, high):
    shape = array.shape
    index_at = [jax.random.randint(jax.random.fold_in(key, axis), (), 0, shape[axis]) for axis in range(len(shape))]
    array = array.at[tuple(index_at)].set(least)
    longest = shape.index(max(shape))
    index_at[longest] = (index_at[longest] + 1) % shape[longest]
    return array.at[tuple(index_at)].set(high)


def block_scale(key, extent, cuts, smallest, high):
    factor_of, own = 1.0, jax.random.fold_in(key, 6)
    for axis_at, parts in cuts:
        heights = jnp.exp(jax.random.uniform(jax.random.fold_in(own, axis_at), (parts,), jnp.float32, smallest / len(cuts), high / len(cuts)))
        factor_of = factor_of * jnp.repeat(heights, extent[axis_at] // parts).reshape([-1 if axis == axis_at else 1 for axis in range(len(extent))])
    return factor_of


def bell_draw(own_key, extent, spread, reach, split=(), held_as=jnp.bfloat16):
    drawn = jax.random.normal(own_key, extent, jnp.float32) * spread
    if len(split) > 0:
        drawn = block_scale(own_key, extent, split, -0.22, 0.18) * drawn
    return jnp.clip(drawn, min=-reach, max=reach).astype(held_as)


def setup_inputs(seed: int = 0) -> dict:
    streams_of = jax.random.split(jax.random.key(seed), 9)
    return {
        "queries": draw_queries(jax.random.fold_in(streams_of[8], 71), 0),
        "prefix_keys": bell_draw(streams_of[1], (PREFIX, KV_HEADS * HEAD_DIM), 1.0, 4.0, ((0, 8),)),
        "prefix_values": bell_draw(streams_of[2], (PREFIX, KV_HEADS * HEAD_DIM), 1.0, 4.0, ((0, 8),)),
        "suffix_keys": draw_suffix_keys(jax.random.fold_in(streams_of[8], 71), 0),
        "suffix_values": bell_draw(streams_of[4], (SAMPLES, SUFFIX, KV_HEADS * HEAD_DIM), 1.0, 4.0, ((0, 4), (1, 8))),
        "layout_pre": plant((jax.random.randint(streams_of[5], (SAMPLES, SUF_BLOCKS, PRE_BLOCKS), 0, 3) < 1).astype(jnp.int32), jax.random.fold_in(streams_of[5], 1), 0, 1),
        "layout_suf": plant((jax.random.randint(streams_of[6], (SAMPLES, SUF_BLOCKS, SUF_BLOCKS), 0, 2) < 1).astype(jnp.int32), jax.random.fold_in(streams_of[6], 1), 0, 1),
        "lengths": plant(jax.random.randint(streams_of[7], (SAMPLES,), 1, SUF_BLOCKS + 1), jax.random.fold_in(streams_of[7], 1), 1, SUF_BLOCKS).astype(jnp.int32),
    }


masked_value = -1e+30

def reference(queries, prefix_keys, prefix_values, suffix_keys, suffix_values, layout_pre, layout_suf, lengths):
    group_size = HEADS // KV_HEADS
    score_scale = 1.0 / math.sqrt(HEAD_DIM)
    prefix_key_rows = prefix_keys.astype(jnp.float32).reshape(PREFIX, KV_HEADS, HEAD_DIM)
    prefix_value_rows = prefix_values.astype(jnp.float32).reshape(PREFIX, KV_HEADS, HEAD_DIM)
    prefix_block = jnp.arange(PREFIX, dtype=jnp.int32) // BLOCK
    suffix_position = jnp.arange(SUFFIX, dtype=jnp.int32)
    suffix_block = suffix_position // BLOCK

    def one_block(flat_index):
        sample = flat_index // SUF_BLOCKS
        block_index = flat_index % SUF_BLOCKS
        query_rows = lax.dynamic_slice_in_dim(queries[sample], (block_index * BLOCK).astype(jnp.int32), BLOCK, 0)
        query_grid = query_rows.astype(jnp.float32).reshape(BLOCK, KV_HEADS, group_size, HEAD_DIM)
        key_rows = jnp.concatenate([prefix_key_rows, suffix_keys[sample].astype(jnp.float32).reshape(SUFFIX, KV_HEADS, HEAD_DIM)], axis=0)
        value_rows = jnp.concatenate([prefix_value_rows, suffix_values[sample].astype(jnp.float32).reshape(SUFFIX, KV_HEADS, HEAD_DIM)], axis=0)
        scores = jnp.einsum('qgjd,lgd->gjql', query_grid, key_rows) * score_scale
        prefix_seen = layout_pre[sample, block_index][prefix_block] > 0
        query_position = block_index * BLOCK + jnp.arange(BLOCK, dtype=jnp.int32)
        suffix_seen = ((suffix_block == block_index) | (layout_suf[sample, block_index][suffix_block] > 0))[None, :]
        suffix_seen = suffix_seen & (suffix_position[None, :] <= query_position[:, None])
        key_mask = jnp.concatenate([jnp.broadcast_to(prefix_seen[None, :], (BLOCK, PREFIX)), suffix_seen], axis=1)
        row_max = lax.optimization_barrier(jnp.max(jnp.where(key_mask, scores, masked_value), axis=-1, keepdims=True))
        weights = jnp.where(key_mask, jnp.exp(scores - row_max), 0.0)
        run_total = lax.optimization_barrier(jnp.sum(weights, axis=-1))
        rounded = lax.optimization_barrier(weights.astype(jnp.bfloat16)).astype(jnp.float32)
        mixed = jnp.einsum('gjql,lgd->qgjd', rounded, value_rows) / jnp.transpose(run_total, (2, 0, 1))[..., None]
        is_live = block_index < lengths[sample]
        return jnp.where(is_live, mixed.reshape(BLOCK, HEADS * HEAD_DIM), 0.0).astype(jnp.bfloat16)
    blocks = lax.map(one_block, jnp.arange(SAMPLES * SUF_BLOCKS, dtype=jnp.int32))
    return blocks.reshape(SAMPLES, SUFFIX, HEADS * HEAD_DIM)
```

```python
import functools
import math

import jax
import jax.numpy as jnp
from jax import lax
from jax.experimental import pallas as pl
from jax.experimental.pallas import tpu as pltpu
from jax.sharding import PartitionSpec as P

HEADS = 40
KV_HEADS = 8
HEAD_DIM = 128
BLOCK = 128
GROUP = HEADS // KV_HEADS
WIDE = GROUP * BLOCK
COLUMNS = 2


masked_value = -1e30
exponent_scale = math.log2(math.e) / math.sqrt(HEAD_DIM)


def pack(keys, values):
    key_part = keys.reshape(BLOCK, KV_HEADS, HEAD_DIM).transpose(1, 0, 2)
    value_part = values.reshape(BLOCK, KV_HEADS, HEAD_DIM).transpose(1, 2, 0)
    return jnp.stack([key_part, value_part], axis=1)


def head_of(step, samp_index, shares):
    per_share = KV_HEADS // shares
    half = KV_HEADS // 2
    core_rel = step // half
    inner = step % half
    x_rel = inner // per_share
    share = samp_index ^ (x_rel * 2 + core_rel)
    return share * per_share + inner % per_share


def attend_kernel(suffix_count, prefix_count, scalars, query_ref, *refs):
    suffix_refs = refs[:suffix_count]
    near_ref, far_ref = refs[suffix_count : suffix_count + 2]
    out_ref = refs[suffix_count + 2]
    score_ref, peak_ref, sum_ref, total_ref = refs[suffix_count + 3 :]
    step = pl.program_id(0)
    half = KV_HEADS // 2
    live = scalars[1]
    base = 2

    @pl.when(live > 0)
    def compute():
        queries = jnp.concatenate(
            [query_ref[:, j * HEAD_DIM : (j + 1) * HEAD_DIM] for j in range(GROUP)], axis=0
        )
        peak_ref[...] = jnp.full_like(peak_ref, masked_value)
        sum_ref[...] = jnp.zeros_like(sum_ref)
        total_ref[...] = jnp.zeros_like(total_ref)

        def first(keys, slot, diagonal):
            scores = lax.dot_general(
                keys, queries, (((1,), (1,)), ((), ())), preferred_element_type=jnp.float32
            )
            if diagonal:
                key_at = lax.broadcasted_iota(jnp.int32, (BLOCK, WIDE), 0)
                query_at = lax.broadcasted_iota(jnp.int32, (BLOCK, WIDE), 1) % BLOCK
                scores = jnp.where(key_at <= query_at, scores, masked_value)
            score_ref[slot] = scores
            peak_ref[...] = jnp.maximum(
                peak_ref[...], jnp.max(scores.reshape(BLOCK // 8, 8, WIDE), axis=0)
            )

        def second(values, slot, peak):
            weights = jnp.exp2((score_ref[slot] - peak) * exponent_scale)
            sum_ref[...] += jnp.sum(weights.reshape(BLOCK // 8, 8, WIDE), axis=0)
            total_ref[...] += lax.dot_general(
                values,
                weights.astype(jnp.bfloat16),
                (((1,), (0,)), ((), ())),
                preferred_element_type=jnp.float32,
            )

        first(suffix_refs[0][0], 0, True)
        for n in range(1, suffix_count):

            @pl.when(scalars[base + n] > 0)
            def _(n=n):
                first(suffix_refs[n][0], n, False)

        for ref, here in ((near_ref, step < half), (far_ref, step >= half)):

            @pl.when(here)
            def _(ref=ref):
                def body(n, unused):
                    @pl.when(scalars[base + suffix_count + n] > 0)
                    def _():
                        first(ref[n, 0], suffix_count + n, False)

                    return unused

                lax.fori_loop(0, prefix_count, body, 0)

        peak = jnp.max(peak_ref[...], axis=0, keepdims=True)
        second(suffix_refs[0][1], 0, peak)
        for n in range(1, suffix_count):

            @pl.when(scalars[base + n] > 0)
            def _(n=n):
                second(suffix_refs[n][1], n, peak)

        for ref, here in ((near_ref, step < half), (far_ref, step >= half)):

            @pl.when(here)
            def _(ref=ref):
                def body(n, unused):
                    @pl.when(scalars[base + suffix_count + n] > 0)
                    def _():
                        second(ref[n, 1], suffix_count + n, peak)

                    return unused

                lax.fori_loop(0, prefix_count, body, 0)

        denominator = jnp.sum(sum_ref[...], axis=0, keepdims=True)
        mixed = total_ref[...] / denominator
        for j in range(GROUP):
            out_ref[:, j * HEAD_DIM : (j + 1) * HEAD_DIM] = mixed[
                :, j * BLOCK : (j + 1) * BLOCK
            ].T.astype(jnp.bfloat16)

    @pl.when(live == 0)
    def blank():
        out_ref[...] = jnp.zeros_like(out_ref)


def attend(scalars, queries, suffix_blocks, near, far, shares):
    suffix_count = len(suffix_blocks)
    prefix_count = near.shape[1]
    per_share = KV_HEADS // shares
    half = KV_HEADS // 2

    def by_head(step, scalars):
        return head_of(step, scalars[0], shares)

    def near_at(step, scalars):
        inner = jnp.minimum(step, half - 1)
        return (inner // per_share, 0, inner % per_share, 0, 0, 0)

    def far_at(step, scalars):
        inner = jnp.maximum(step, half) - half
        return (inner // per_share, 0, inner % per_share, 0, 0, 0)

    prefix_block = (None, prefix_count, None, 2, BLOCK, HEAD_DIM)
    blocks = suffix_count + prefix_count
    return pl.pallas_call(
        functools.partial(attend_kernel, suffix_count, prefix_count),
        out_shape=jax.ShapeDtypeStruct((BLOCK, HEADS * HEAD_DIM), jnp.bfloat16),
        grid_spec=pltpu.PrefetchScalarGridSpec(
            num_scalar_prefetch=1,
            grid=(KV_HEADS,),
            in_specs=[pl.BlockSpec((BLOCK, WIDE), lambda t, s: (0, by_head(t, s)))]
            + [
                pl.BlockSpec((None, 2, BLOCK, HEAD_DIM), lambda t, s: (by_head(t, s), 0, 0, 0))
                for _ in range(suffix_count)
            ]
            + [pl.BlockSpec(prefix_block, near_at), pl.BlockSpec(prefix_block, far_at)],
            out_specs=pl.BlockSpec((BLOCK, WIDE), lambda t, s: (0, by_head(t, s))),
            scratch_shapes=[
                pltpu.VMEM((blocks, BLOCK, WIDE), jnp.float32),
                pltpu.VMEM((8, WIDE), jnp.float32),
                pltpu.VMEM((8, WIDE), jnp.float32),
                pltpu.VMEM((HEAD_DIM, WIDE), jnp.float32),
            ],
        ),
        name="attend",
    )(scalars, queries, *suffix_blocks, near, far)


def shards(
    queries, prefix_keys, prefix_values, suffix_keys, suffix_values, layout_pre, layout_suf, lengths
):
    seq_count = lax.axis_size("seq")
    shares = lax.axis_size("samp")
    rows = seq_count // COLUMNS
    seq_index = lax.axis_index("seq")
    samp_index = lax.axis_index("samp")
    row, column = seq_index // COLUMNS, seq_index % COLUMNS
    per_share = KV_HEADS // shares

    def at(z, y):
        return z * COLUMNS + y

    def along_rows(pairs):
        return [(at(a, y), at(b, y)) for a, b in pairs for y in range(COLUMNS)]

    def move(value, pairs, axis="seq"):
        return lax.ppermute(value, axis, pairs)

    swap_columns = [(i, i ^ 1) for i in range(seq_count)]
    upward = along_rows([(z, z + 1) for z in range(rows - 1)])
    to_top = along_rows([(0, rows - 1)])

    own = pack(suffix_keys[0], suffix_values[0])
    packed_prefix = pack(prefix_keys, prefix_values)
    own_share = lax.dynamic_slice_in_dim(packed_prefix, samp_index * per_share, per_share, 0)

    chain = [own]
    cross = [move(own, swap_columns)]
    for k in range(1, rows):
        if k < rows - 1 or rows == 2:
            chain.append(move(chain[-1], upward))
            cross.append(move(chain[-1], swap_columns))
        else:
            chain.append(move(own, to_top))
            cross.append(move(cross[0], to_top))

    gathered = [own_share]
    for k in range(1, rows):
        gathered.append(
            move(own_share, along_rows([(z, (z + k) % rows) for z in range(rows)]))
        )
    same = jnp.stack(gathered)
    swap_x = [(i, i ^ 2) for i in range(shares)]
    swap_core = [(i, i ^ 1) for i in range(shares)]
    other = move(same, swap_columns)
    same_x = move(same, swap_x, "samp")
    other_x = move(other, swap_x, "samp")
    near = jnp.stack([jnp.concatenate([same, other]), jnp.concatenate([same_x, other_x])])
    far = move(near, swap_core, "samp")

    pre_row = layout_pre[0, 0, :]
    suf_row = layout_suf[0, 0, :]
    distance = jnp.arange(rows, dtype=jnp.int32)
    prefix_at = jnp.concatenate(
        [((row - distance) % rows) * COLUMNS + y for y in (column, 1 - column)]
    )
    suffix_at = jnp.concatenate(
        [(row - distance) * COLUMNS + y for y in (column, 1 - column)]
    )
    prefix_seen = pre_row[prefix_at] > 0
    suffix_seen = (
        (suffix_at >= 0)
        & (suffix_at < seq_index)
        & (suf_row[jnp.maximum(suffix_at, 0)] > 0)
    )
    suffix_seen = suffix_seen.at[0].set(True)
    live = seq_index < lengths[0]
    scalars = jnp.concatenate(
        [
            samp_index[None],
            live.astype(jnp.int32)[None],
            suffix_seen.astype(jnp.int32),
            prefix_seen.astype(jnp.int32),
        ]
    ).astype(jnp.int32)
    out = attend(scalars, queries[0], chain + cross, near, far, shares)
    return out[None]


def solution(mesh):
    return jax.shard_map(
        shards,
        mesh=mesh,
        in_specs=(
            P("samp", "seq", None),
            P("seq", None),
            P("seq", None),
            P("samp", "seq", None),
            P("samp", "seq", None),
            P("samp", "seq", None),
            P("samp", "seq", None),
            P("samp"),
        ),
        out_specs=P("samp", "seq", None),
        check_vma=False,
    )
```

```python
import functools
import math

import jax
import jax.numpy as jnp
from jax import lax
from jax.experimental import pallas as pl
from jax.experimental.pallas import tpu as pltpu
from jax.sharding import PartitionSpec as P


HEADS = 40
KV_HEADS = 8
HEAD_DIM = 128
BLOCK = 128
GROUP = HEADS // KV_HEADS
WIDE = GROUP * BLOCK
COLUMNS = 2
TOGETHER = 2
CHUNK = 4


masked_value = -1e30
exponent_scale = math.log2(math.e) / math.sqrt(HEAD_DIM)


def pack_kernel(heads, first_ref, key_ref, value_ref, out_ref):
    for n in range(heads):
        lanes = pl.ds(pl.multiple_of((first_ref[0] + n) * HEAD_DIM, HEAD_DIM), HEAD_DIM)
        out_ref[n, 0] = key_ref[:, lanes]
        out_ref[n, 1] = value_ref[:, lanes].T


def pack(keys, values, first_head, heads):
    inside = pl.BlockSpec(memory_space=pltpu.VMEM)
    return pl.pallas_call(
        functools.partial(pack_kernel, heads),
        out_shape=pltpu.VMEM((heads, 2, BLOCK, HEAD_DIM), keys.dtype),
        in_specs=[pl.BlockSpec(memory_space=pltpu.SMEM), inside, inside],
        out_specs=inside,
        compiler_params=pltpu.CompilerParams(vmem_limit_bytes=4 * 2**20),
        name="pack",
    )(
        first_head,
        pltpu.with_memory_space_constraint(keys, pltpu.VMEM),
        pltpu.with_memory_space_constraint(values, pltpu.VMEM),
    )


def head_of(step, samp_index, shares):
    per_share = KV_HEADS // shares
    half = KV_HEADS // 2
    core_rel = step // half
    inner = step % half
    x_rel = inner // per_share
    share = samp_index ^ (x_rel * 2 + core_rel)
    return share * per_share + inner % per_share


def attend_kernel(plan, place, pre_row, suf_row, lengths, query_ref, *refs):
    slots, prefix_count, rows, shares, first, last = plan
    refs = list(refs)
    block_refs = [[refs.pop(0) for _ in range(parts)] for slot, parts in slots]
    slots = [slot for slot, parts in slots]
    prefix_refs = [refs.pop(0) for _ in range(8)] if prefix_count else []
    state_ref = None if first else refs.pop(0)
    out_ref = refs.pop(0)
    if first or not last:
        state_ref = out_ref
    key_buffer, value_buffer, seen_list = refs
    half = KV_HEADS // 2
    per_share = KV_HEADS // shares
    seq_index, samp_index = place[0], place[1]
    row, column = seq_index // COLUMNS, seq_index % COLUMNS
    live = seq_index < lengths[0]

    def suffix_seen(slot):
        back, across = slot
        side = 1 - column if across else column
        block = (row - back) * COLUMNS + side
        inside = (block >= 0) & (block < seq_index)
        return inside & (suf_row[jnp.maximum(block, 0)] > 0)

    def prefix_seen(n):
        side = jnp.where(n >= rows, 1 - column, column)
        back = n % rows
        block = jnp.where(row >= back, row - back, row - back + rows) * COLUMNS + side
        return pre_row[block] > 0

    @pl.when(live)
    def compute():
        places, suffix_end = [], jnp.int32(0)
        for slot in slots:
            seen = True if slot == (0, False) else suffix_seen(slot)
            places.append((seen, suffix_end))
            suffix_end = suffix_end + (1 if seen is True else seen.astype(jnp.int32))
        near_count = prefix_seen_count = jnp.int32(0)
        if prefix_count:

            def note(n, found):
                seen_list[found] = n
                return found + prefix_seen(n).astype(jnp.int32)

            near_count = lax.fori_loop(0, rows, note, jnp.int32(0))
            prefix_seen_count = lax.fori_loop(rows, prefix_count, note, near_count)
        count = suffix_end + prefix_seen_count

        def some_heads(turn, unused):
            step = turn * TOGETHER
            head = head_of(step, samp_index, shares)
            inner = step % half
            lanes = range(TOGETHER)

            def take(position, sources):
                for i, source in enumerate(sources):
                    key_buffer[i, position] = source[0]
                    value_buffer[i, position] = source[1]

            def take_block(n, position):
                parts = block_refs[n]
                height = KV_HEADS // len(parts)
                for m, part in enumerate(parts):

                    @pl.when((head >= m * height) & (head < (m + 1) * height))
                    def _(m=m, part=part):
                        take(position, [part.at[head - m * height + i] for i in lanes])

            for n, (seen, position) in enumerate(places):
                if seen is True:
                    take_block(n, position)
                else:
                    pl.when(seen)(functools.partial(take_block, n, position))

            for way in range(4 if prefix_count else 0):
                pieces = prefix_refs[way * 2 : way * 2 + 2]

                def take_prefix(ref, skipped, n, unused):
                    chosen = ref.at[seen_list[n] - skipped]
                    first_head = inner % per_share
                    take(suffix_end + n, [chosen.at[first_head + i] for i in lanes])
                    return unused

                @pl.when(step // per_share == way)
                def _(pieces=pieces):
                    lax.fori_loop(0, near_count, functools.partial(take_prefix, pieces[0], 0), 0)
                    lax.fori_loop(
                        near_count,
                        prefix_seen_count,
                        functools.partial(take_prefix, pieces[1], rows),
                        0,
                    )

            offset = pl.multiple_of(head * WIDE, WIDE)
            wide = query_ref[:, pl.ds(offset, TOGETHER * WIDE)]
            queries = [
                jnp.concatenate(
                    [
                        wide[:, (i * GROUP + j) * HEAD_DIM : (i * GROUP + j + 1) * HEAD_DIM]
                        for j in range(GROUP)
                    ],
                    axis=0,
                )
                for i in lanes
            ]
            state = [state_ref.at[step + i] for i in lanes]
            sums = slice(HEAD_DIM + 8, HEAD_DIM + 16)

            def chunk(start, size, fresh):
                keys = [
                    key_buffer[i, pl.ds(start, size)].reshape(size * BLOCK, HEAD_DIM)
                    for i in lanes
                ]
                values = [
                    jnp.concatenate([value_buffer[i, start + n] for n in range(size)], axis=1)
                    for i in lanes
                ]
                before = [None if fresh else state[i][HEAD_DIM:] for i in lanes]
                tall = size * BLOCK // 8
                after = []
                for i in lanes:
                    scores = lax.dot_general(
                        keys[i],
                        queries[i],
                        (((1,), (1,)), ((), ())),
                        preferred_element_type=jnp.float32,
                    )
                    if fresh:
                        key_at = lax.broadcasted_iota(jnp.int32, (BLOCK, WIDE), 0)
                        query_at = lax.broadcasted_iota(jnp.int32, (BLOCK, WIDE), 1) % BLOCK
                        scores = jnp.where(key_at <= query_at, scores, masked_value)
                    new = jnp.max(scores, axis=0, keepdims=True)
                    if not fresh:
                        new = jnp.maximum(before[i][0:1], new)
                    weights = jnp.exp2((scores - new) * exponent_scale)
                    part_sum = jnp.sum(weights.reshape(tall, 8, WIDE), axis=0)
                    part = lax.dot_general(
                        values[i],
                        weights.astype(jnp.bfloat16),
                        (((1,), (0,)), ((), ())),
                        preferred_element_type=jnp.float32,
                    )
                    after.append((new, part_sum, part))
                for i in lanes:
                    new, part_sum, part = after[i]
                    if not fresh:
                        shrink = jnp.exp2((before[i][0:1] - new) * exponent_scale)
                        part_sum = part_sum + before[i][8:] * shrink
                        part = part + state[i][:HEAD_DIM] * shrink
                    state[i][:HEAD_DIM] = part
                    state[i][HEAD_DIM : HEAD_DIM + 8] = jnp.broadcast_to(new, (8, WIDE))
                    state[i][sums] = part_sum

            start = 0
            if first:
                chunk(0, 1, True)
                start = 1
            rest = count - start

            def many(n, unused):
                chunk(start + n * CHUNK, CHUNK, False)
                return unused

            largest = len(slots) + prefix_count - start
            if largest >= CHUNK:
                lax.fori_loop(0, rest // CHUNK, many, 0)
            size = CHUNK // 2
            while size:
                if largest >= size:

                    @pl.when(rest // size % 2 == 1)
                    def _(size=size):
                        chunk(start + rest // (2 * size) * (2 * size), size, False)

                size //= 2

            if last:
                parts = []
                for i in lanes:
                    inverse = 1.0 / jnp.sum(state[i][sums], axis=0, keepdims=True)
                    mixed = (state[i][:HEAD_DIM] * inverse).astype(jnp.bfloat16)
                    parts += [mixed[:, j * BLOCK : (j + 1) * BLOCK].T for j in range(GROUP)]
                out_ref[:, pl.ds(offset, TOGETHER * WIDE)] = jnp.concatenate(parts, axis=1)
            return unused

        lax.fori_loop(0, KV_HEADS // TOGETHER, some_heads, 0)

    if last:

        @pl.when(jnp.logical_not(live))
        def blank():
            out_ref[...] = jnp.zeros_like(out_ref)


def attend(tables, queries, slots, blocks, prefix, state, shares, rows, last):
    prefix_count = prefix[0].shape[0] * COLUMNS if prefix else 0
    first = state is None
    total = len(slots) + prefix_count
    plan = tuple((slot, len(parts)) for slot, parts in zip(slots, blocks))
    blocks = [part for parts in blocks for part in parts]
    state_shape = (KV_HEADS, HEAD_DIM + 16, WIDE)
    if last:
        out_shape = jax.ShapeDtypeStruct((BLOCK, HEADS * HEAD_DIM), jnp.bfloat16)
    else:
        out_shape = pltpu.VMEM(state_shape, jnp.float32)
    operands = [queries, *blocks, *prefix] + ([] if first else [state])
    operands = [pltpu.with_memory_space_constraint(x, pltpu.VMEM) for x in operands]
    inside = pl.BlockSpec(memory_space=pltpu.VMEM)
    table = pl.BlockSpec(memory_space=pltpu.SMEM)
    aliases = {} if first or last else {len(tables) + len(operands) - 1: 0}
    return pl.pallas_call(
        functools.partial(
            attend_kernel, (plan, prefix_count, rows, shares, first, last)
        ),
        out_shape=out_shape,
        in_specs=[table] * len(tables) + [inside] * len(operands),
        out_specs=inside,
        scratch_shapes=[
            pltpu.VMEM((TOGETHER, total, BLOCK, HEAD_DIM), jnp.bfloat16),
            pltpu.VMEM((TOGETHER, total, HEAD_DIM, BLOCK), jnp.bfloat16),
            pltpu.SMEM((max(prefix_count, 1) + 1,), jnp.int32),
        ],
        input_output_aliases=aliases,
        compiler_params=pltpu.CompilerParams(vmem_limit_bytes=10 * 2**20 + total * 2**17),
    )(*tables, *operands)


def shards(
    queries, prefix_keys, prefix_values, suffix_keys, suffix_values, layout_pre, layout_suf, lengths
):
    seq_count = lax.axis_size("seq")
    shares = lax.axis_size("samp")
    rows = seq_count // COLUMNS
    seq_index = lax.axis_index("seq")
    samp_index = lax.axis_index("samp")
    per_share = KV_HEADS // shares

    def along_rows(pairs):
        return [(a * COLUMNS + y, b * COLUMNS + y) for a, b in pairs for y in range(COLUMNS)]

    def move(value, pairs, axis="seq"):
        return lax.ppermute(value, axis, pairs)

    swap_columns = [(i, i ^ 1) for i in range(seq_count)]
    own = pack(suffix_keys[0], suffix_values[0], jnp.zeros(1, jnp.int32), KV_HEADS)
    first_head = (samp_index * per_share).astype(jnp.int32)
    own_share = pack(prefix_keys, prefix_values, first_head[None], per_share)

    held = {(0, False): own}
    across = [(z * COLUMNS, z * COLUMNS + 1) for z in range(rows)]
    held[0, True] = move(own, across)
    for k in range(1, rows):
        upward = along_rows([(z, z + 1) for z in range(k - 1, rows - 1)])
        held[k, False] = move(held[k - 1, False], upward)
        if k < rows - 1:
            held[k, True] = move(held[k, False], swap_columns[k * COLUMNS :])
    low = slice(0, KV_HEADS // 2)
    high = slice(KV_HEADS // 2, KV_HEADS)
    top = rows - 1
    from_side = move(held[top, False][low], swap_columns[top * COLUMNS :])
    source = held[top - 1, True] if top > 1 else move(own, [(1, 0)] + across[:1])
    from_below = move(source[high], along_rows([(top - 1, top)]))
    held[top, True] = (from_side, from_below)

    gathered = [own_share]
    for k in range(1, rows):
        turn = along_rows([(z, (z + k) % rows) for z in range(rows)])
        gathered.append(move(own_share, turn))
    swap_x = [(i, i ^ 2) for i in range(shares)]
    swap_core = [(i, i ^ 1) for i in range(shares)]
    same = jnp.stack(gathered)
    other = move(same, swap_columns)
    same_x = move(same, swap_x, "samp")
    other_x = move(other, swap_x, "samp")
    near = [same, other, same_x, other_x]
    far = [move(piece, swap_core, "samp") for piece in near]

    early, late = stages(rows)
    middle = [slot for slot in held if slot not in early and slot not in late]
    tables = (
        jnp.stack([seq_index, samp_index]).astype(jnp.int32),
        layout_pre[0, 0],
        layout_suf[0, 0],
        lengths,
    )

    def run(slots, prefix, state, last):
        blocks = [held[slot] if isinstance(held[slot], tuple) else (held[slot],) for slot in slots]
        return attend(tables, queries[0], slots, blocks, prefix, state, shares, rows, last)

    state = run(early, [], None, False)
    state = run(middle, near + far, state, False)
    return run(late, [], state, True)[None]


def stages(rows):
    early = [(0, False), (0, True)] + [(1, False)] * (rows > 2)
    late = [(rows - 1, False), (rows - 1, True)]
    if rows > 2:
        late.insert(0, (rows - 2, True))
    return early, [slot for slot in late if slot not in early]


def solution(mesh):
    return jax.shard_map(
        shards,
        mesh=mesh,
        in_specs=(
            P("samp", "seq", None),
            P("seq", None),
            P("seq", None),
            P("samp", "seq", None),
            P("samp", "seq", None),
            P("samp", "seq", None),
            P("samp", "seq", None),
            P("samp"),
        ),
        out_specs=P("samp", "seq", None),
        check_vma=False,
    )
```

```python
import functools
import math

import jax
import jax.numpy as jnp
from jax import lax
from jax.experimental import pallas as pl
from jax.experimental.pallas import tpu as pltpu
from jax.sharding import PartitionSpec as P


HEADS = 40
KV_HEADS = 8
HEAD_DIM = 128
BLOCK = 128
GROUP = HEADS // KV_HEADS
WIDE = GROUP * BLOCK
COLUMNS = 2
TOGETHER = 2
CHUNK = 4


masked_value = -1e30
exponent_scale = math.log2(math.e) / math.sqrt(HEAD_DIM)


def pack_kernel(first_ref, *refs):
    sources, outs = refs[:4], refs[4:6]
    wides, narrows, semaphores = refs[6], refs[7], refs[8]
    heads = outs[1].shape[0]
    lanes = pl.ds(pl.multiple_of(first_ref[0] * HEAD_DIM, HEAD_DIM), heads * HEAD_DIM)
    copies = [
        pltpu.make_async_copy(sources[n].at[:, lanes], narrows.at[n], semaphores.at[n])
        for n in range(2)
    ] + [
        pltpu.make_async_copy(sources[n + 2], wides.at[n], semaphores.at[n + 2])
        for n in range(2)
    ]
    for copy in copies:
        copy.start()
    for out, held, pair in ((outs[1], narrows, copies[:2]), (outs[0], wides, copies[2:])):
        for copy in pair:
            copy.wait()
        for n in range(out.shape[0]):
            out[n, 0] = held[0, :, n * HEAD_DIM : (n + 1) * HEAD_DIM]
            out[n, 1] = held[1, :, n * HEAD_DIM : (n + 1) * HEAD_DIM].T


def pack(suffix_keys, suffix_values, prefix_keys, prefix_values, first_head, heads):
    kind = suffix_keys.dtype
    width = KV_HEADS * HEAD_DIM
    return pl.pallas_call(
        pack_kernel,
        out_shape=(
            pltpu.VMEM((KV_HEADS, 2, BLOCK, HEAD_DIM), kind),
            pltpu.VMEM((heads, 2, BLOCK, HEAD_DIM), kind),
        ),
        in_specs=[pl.BlockSpec(memory_space=pltpu.SMEM)]
        + [pl.BlockSpec(memory_space=pltpu.HBM)] * 4,
        out_specs=[pl.BlockSpec(memory_space=pltpu.VMEM)] * 2,
        scratch_shapes=[
            pltpu.VMEM((2, BLOCK, width), kind),
            pltpu.VMEM((2, BLOCK, heads * HEAD_DIM), kind),
            pltpu.SemaphoreType.DMA((4,)),
        ],
        compiler_params=pltpu.CompilerParams(vmem_limit_bytes=6 * 2**20),
        name="pack",
    )(
        first_head,
        *(
            pltpu.with_memory_space_constraint(x, pltpu.HBM)
            for x in (prefix_keys, prefix_values, suffix_keys, suffix_values)
        ),
    )


def head_of(step, samp_index, shares):
    per_share = KV_HEADS // shares
    half = KV_HEADS // 2
    core_rel = step // half
    inner = step % half
    x_rel = inner // per_share
    share = samp_index ^ (x_rel * 2 + core_rel)
    return share * per_share + inner % per_share


def attend_kernel(plan, place, pre_row, suf_row, lengths, query_ref, *refs):
    slots, prefix_count, rows, shares, first, last = plan
    refs = list(refs)
    block_refs = [[refs.pop(0) for _ in range(parts)] for slot, parts in slots]
    slots = [slot for slot, parts in slots]
    prefix_refs = [refs.pop(0) for _ in range(8)] if prefix_count else []
    state_ref = None if first else refs.pop(0)
    out_ref = refs.pop(0)
    if first or not last:
        state_ref = out_ref
    key_buffer, value_buffer, seen_list = refs
    half = KV_HEADS // 2
    per_share = KV_HEADS // shares
    seq_index, samp_index = place[0], place[1]
    row, column = seq_index // COLUMNS, seq_index % COLUMNS
    live = seq_index < lengths[0]

    def suffix_seen(slot):
        back, across = slot
        side = 1 - column if across else column
        block = (row - back) * COLUMNS + side
        inside = (block >= 0) & (block < seq_index)
        return inside & (suf_row[jnp.maximum(block, 0)] > 0)

    def prefix_seen(n):
        side = jnp.where(n >= rows, 1 - column, column)
        back = n % rows
        block = jnp.where(row >= back, row - back, row - back + rows) * COLUMNS + side
        return pre_row[block] > 0

    @pl.when(live)
    def compute():
        places, suffix_end = [], jnp.int32(0)
        for slot in slots:
            seen = True if slot == (0, False) else suffix_seen(slot)
            places.append((seen, suffix_end))
            suffix_end = suffix_end + (1 if seen is True else seen.astype(jnp.int32))
        near_count = prefix_seen_count = jnp.int32(0)
        if prefix_count:

            def note(n, found):
                seen_list[found] = n
                return found + prefix_seen(n).astype(jnp.int32)

            near_count = lax.fori_loop(0, rows, note, jnp.int32(0))
            prefix_seen_count = lax.fori_loop(rows, prefix_count, note, near_count)
        count = suffix_end + prefix_seen_count

        def some_heads(turn, unused):
            step = turn * TOGETHER
            head = head_of(step, samp_index, shares)
            inner = step % half
            lanes = range(TOGETHER)

            def take(position, sources):
                for i, source in enumerate(sources):
                    key_buffer[i, position] = source[0]
                    value_buffer[i, position] = source[1]

            def take_block(n, position):
                parts = block_refs[n]
                height = KV_HEADS // len(parts)
                for m, part in enumerate(parts):

                    @pl.when((head >= m * height) & (head < (m + 1) * height))
                    def _(m=m, part=part):
                        take(position, [part.at[head - m * height + i] for i in lanes])

            for n, (seen, position) in enumerate(places):
                if seen is True:
                    take_block(n, position)
                else:
                    pl.when(seen)(functools.partial(take_block, n, position))

            for way in range(4 if prefix_count else 0):
                pieces = prefix_refs[way * 2 : way * 2 + 2]

                def take_prefix(ref, skipped, n, unused):
                    chosen = ref.at[seen_list[n] - skipped]
                    first_head = inner % per_share
                    take(suffix_end + n, [chosen.at[first_head + i] for i in lanes])
                    return unused

                @pl.when(step // per_share == way)
                def _(pieces=pieces):
                    lax.fori_loop(0, near_count, functools.partial(take_prefix, pieces[0], 0), 0)
                    lax.fori_loop(
                        near_count,
                        prefix_seen_count,
                        functools.partial(take_prefix, pieces[1], rows),
                        0,
                    )

            offset = pl.multiple_of(head * WIDE, WIDE)
            wide = query_ref[:, pl.ds(offset, TOGETHER * WIDE)]
            queries = [
                jnp.concatenate(
                    [
                        wide[:, (i * GROUP + j) * HEAD_DIM : (i * GROUP + j + 1) * HEAD_DIM]
                        for j in range(GROUP)
                    ],
                    axis=0,
                )
                for i in lanes
            ]
            state = [state_ref.at[step + i] for i in lanes]
            sums = slice(HEAD_DIM + 8, HEAD_DIM + 16)

            def chunk(start, size, fresh):
                keys = [
                    key_buffer[i, pl.ds(start, size)].reshape(size * BLOCK, HEAD_DIM)
                    for i in lanes
                ]
                values = [
                    jnp.concatenate([value_buffer[i, start + n] for n in range(size)], axis=1)
                    for i in lanes
                ]
                before = [None if fresh else state[i][HEAD_DIM:] for i in lanes]
                tall = size * BLOCK // 8
                after = []
                for i in lanes:
                    scores = lax.dot_general(
                        keys[i],
                        queries[i],
                        (((1,), (1,)), ((), ())),
                        preferred_element_type=jnp.float32,
                    )
                    if fresh:
                        key_at = lax.broadcasted_iota(jnp.int32, (BLOCK, WIDE), 0)
                        query_at = lax.broadcasted_iota(jnp.int32, (BLOCK, WIDE), 1) % BLOCK
                        scores = jnp.where(key_at <= query_at, scores, masked_value)
                    new = jnp.max(scores, axis=0, keepdims=True)
                    if not fresh:
                        new = jnp.maximum(before[i][0:1], new)
                    weights = jnp.exp2((scores - new) * exponent_scale)
                    part_sum = jnp.sum(weights.reshape(tall, 8, WIDE), axis=0)
                    part = lax.dot_general(
                        values[i],
                        weights.astype(jnp.bfloat16),
                        (((1,), (0,)), ((), ())),
                        preferred_element_type=jnp.float32,
                    )
                    after.append((new, part_sum, part))
                for i in lanes:
                    new, part_sum, part = after[i]
                    if not fresh:
                        shrink = jnp.exp2((before[i][0:1] - new) * exponent_scale)
                        part_sum = part_sum + before[i][8:] * shrink
                        part = part + state[i][:HEAD_DIM] * shrink
                    state[i][:HEAD_DIM] = part
                    state[i][HEAD_DIM : HEAD_DIM + 8] = jnp.broadcast_to(new, (8, WIDE))
                    state[i][sums] = part_sum

            start = 0
            if first:
                chunk(0, 1, True)
                start = 1
            rest = count - start

            def many(n, unused):
                chunk(start + n * CHUNK, CHUNK, False)
                return unused

            largest = len(slots) + prefix_count - start
            if largest >= CHUNK:
                lax.fori_loop(0, rest // CHUNK, many, 0)
            size = CHUNK // 2
            while size:
                if largest >= size:

                    @pl.when(rest // size % 2 == 1)
                    def _(size=size):
                        chunk(start + rest // (2 * size) * (2 * size), size, False)

                size //= 2

            if last:
                parts = []
                for i in lanes:
                    inverse = 1.0 / jnp.sum(state[i][sums], axis=0, keepdims=True)
                    mixed = (state[i][:HEAD_DIM] * inverse).astype(jnp.bfloat16)
                    parts += [mixed[:, j * BLOCK : (j + 1) * BLOCK].T for j in range(GROUP)]
                out_ref[:, pl.ds(offset, TOGETHER * WIDE)] = jnp.concatenate(parts, axis=1)
            return unused

        lax.fori_loop(0, KV_HEADS // TOGETHER, some_heads, 0)

    if last:

        @pl.when(jnp.logical_not(live))
        def blank():
            out_ref[...] = jnp.zeros_like(out_ref)


def attend(tables, queries, slots, blocks, prefix, state, shares, rows, last):
    prefix_count = prefix[0].shape[0] * COLUMNS if prefix else 0
    first = state is None
    total = len(slots) + prefix_count
    plan = tuple((slot, len(parts)) for slot, parts in zip(slots, blocks))
    blocks = [part for parts in blocks for part in parts]
    state_shape = (KV_HEADS, HEAD_DIM + 16, WIDE)
    if last:
        out_shape = jax.ShapeDtypeStruct((BLOCK, HEADS * HEAD_DIM), jnp.bfloat16)
    else:
        out_shape = pltpu.VMEM(state_shape, jnp.float32)
    operands = [queries, *blocks, *prefix] + ([] if first else [state])
    operands = [pltpu.with_memory_space_constraint(x, pltpu.VMEM) for x in operands]
    inside = pl.BlockSpec(memory_space=pltpu.VMEM)
    table = pl.BlockSpec(memory_space=pltpu.SMEM)
    aliases = {} if first or last else {len(tables) + len(operands) - 1: 0}
    return pl.pallas_call(
        functools.partial(
            attend_kernel, (plan, prefix_count, rows, shares, first, last)
        ),
        out_shape=out_shape,
        in_specs=[table] * len(tables) + [inside] * len(operands),
        out_specs=inside,
        scratch_shapes=[
            pltpu.VMEM((TOGETHER, total, BLOCK, HEAD_DIM), jnp.bfloat16),
            pltpu.VMEM((TOGETHER, total, HEAD_DIM, BLOCK), jnp.bfloat16),
            pltpu.SMEM((max(prefix_count, 1) + 1,), jnp.int32),
        ],
        input_output_aliases=aliases,
        compiler_params=pltpu.CompilerParams(vmem_limit_bytes=10 * 2**20 + total * 2**17),
    )(*tables, *operands)


def shards(
    queries, prefix_keys, prefix_values, suffix_keys, suffix_values, layout_pre, layout_suf, lengths
):
    seq_count = lax.axis_size("seq")
    shares = lax.axis_size("samp")
    rows = seq_count // COLUMNS
    seq_index = lax.axis_index("seq")
    samp_index = lax.axis_index("samp")
    per_share = KV_HEADS // shares

    def along_rows(pairs):
        return [(a * COLUMNS + y, b * COLUMNS + y) for a, b in pairs for y in range(COLUMNS)]

    def move(value, pairs, axis="seq"):
        return lax.ppermute(value, axis, pairs)

    swap_columns = [(i, i ^ 1) for i in range(seq_count)]
    first_head = (samp_index * per_share).astype(jnp.int32)
    own, own_share = pack(
        suffix_keys[0], suffix_values[0], prefix_keys, prefix_values, first_head[None], per_share
    )

    held = {(0, False): own}
    top = rows - 1
    across = [(z * COLUMNS, z * COLUMNS + 1) for z in range(rows)]
    held[0, True] = move(own, across)
    for k in range(1, rows):
        upward = along_rows([(z, z + 1) for z in range(k - 1, top)])
        if k < top or top == 1:
            held[k, False] = move(held[k - 1, False], upward)
            held[k, True] = move(held[k, False], swap_columns[k * COLUMNS :])
        else:
            held[k, False] = move(held[1, False], along_rows([(1, top)]))
            held[k, True] = move(held[1, True], along_rows([(1, top)]))

    gathered = [own_share]
    for k in range(1, rows):
        turn = along_rows([(z, (z + k) % rows) for z in range(rows)])
        gathered.append(move(own_share, turn))
    swap_x = [(i, i ^ 2) for i in range(shares)]
    swap_core = [(i, i ^ 1) for i in range(shares)]
    same = jnp.stack(gathered)
    other = move(same, swap_columns)
    same_x = move(same, swap_x, "samp")
    other_x = move(other, swap_x, "samp")
    near = [same, other, same_x, other_x]
    far = [move(piece, swap_core, "samp") for piece in near]

    early, late, latest = stages(rows)
    middle = [slot for slot in held if slot not in early + late + latest]
    tables = (
        jnp.stack([seq_index, samp_index]).astype(jnp.int32),
        layout_pre[0, 0],
        layout_suf[0, 0],
        lengths,
    )

    def run(slots, prefix, state, last):
        blocks = [held[slot] if isinstance(held[slot], tuple) else (held[slot],) for slot in slots]
        return attend(tables, queries[0], slots, blocks, prefix, state, shares, rows, last)

    state = run(early, [], None, False)
    state = run(middle, near + far, state, False)
    if late:
        state = run(late, [], state, False)
    return run(latest, [], state, True)[None]


def stages(rows):
    early = [(0, False), (0, True)] + [(1, False)] * (rows > 2)
    late = [(rows - 2, True), (rows - 1, False)] if rows > 2 else []
    latest = [(rows - 1, True)] + [(rows - 1, False)] * (rows <= 2)
    return early, late, latest


def solution(mesh):
    return jax.shard_map(
        shards,
        mesh=mesh,
        in_specs=(
            P("samp", "seq", None),
            P("seq", None),
            P("seq", None),
            P("samp", "seq", None),
            P("samp", "seq", None),
            P("samp", "seq", None),
            P("samp", "seq", None),
            P("samp"),
        ),
        out_specs=P("samp", "seq", None),
        check_vma=False,
    )
```

```python
import functools
import math

import jax
import jax.numpy as jnp
from jax import lax
from jax.experimental import pallas as pl
from jax.experimental.pallas import tpu as pltpu
from jax.sharding import PartitionSpec as P


HEADS = 40
KV_HEADS = 8
HEAD_DIM = 128
BLOCK = 128
GROUP = HEADS // KV_HEADS
WIDE = GROUP * BLOCK
COLUMNS = 2
TOGETHER = 2
CHUNK = 4


masked_value = -1e30
exponent_scale = math.log2(math.e) / math.sqrt(HEAD_DIM)


def pack_kernel(first_ref, *refs):
    sources, outs = refs[:4], refs[4:6]
    wides, narrows, semaphores = refs[6], refs[7], refs[8]
    heads = outs[1].shape[0]
    lanes = pl.ds(pl.multiple_of(first_ref[0] * HEAD_DIM, HEAD_DIM), heads * HEAD_DIM)
    copies = [
        pltpu.make_async_copy(sources[n].at[:, lanes], narrows.at[n], semaphores.at[n])
        for n in range(2)
    ] + [
        pltpu.make_async_copy(sources[n + 2], wides.at[n], semaphores.at[n + 2])
        for n in range(2)
    ]
    for copy in copies:
        copy.start()
    for out, held, pair in ((outs[1], narrows, copies[:2]), (outs[0], wides, copies[2:])):
        for copy in pair:
            copy.wait()
        for n in range(out.shape[0]):
            out[n, 0] = held[0, :, n * HEAD_DIM : (n + 1) * HEAD_DIM]
            out[n, 1] = held[1, :, n * HEAD_DIM : (n + 1) * HEAD_DIM].T


def pack(suffix_keys, suffix_values, prefix_keys, prefix_values, first_head, heads):
    kind = suffix_keys.dtype
    width = KV_HEADS * HEAD_DIM
    return pl.pallas_call(
        pack_kernel,
        out_shape=(
            pltpu.VMEM((KV_HEADS, 2, BLOCK, HEAD_DIM), kind),
            pltpu.VMEM((heads, 2, BLOCK, HEAD_DIM), kind),
        ),
        in_specs=[pl.BlockSpec(memory_space=pltpu.SMEM)]
        + [pl.BlockSpec(memory_space=pltpu.HBM)] * 4,
        out_specs=[pl.BlockSpec(memory_space=pltpu.VMEM)] * 2,
        scratch_shapes=[
            pltpu.VMEM((2, BLOCK, width), kind),
            pltpu.VMEM((2, BLOCK, heads * HEAD_DIM), kind),
            pltpu.SemaphoreType.DMA((4,)),
        ],
        compiler_params=pltpu.CompilerParams(vmem_limit_bytes=6 * 2**20),
        name="pack",
    )(
        first_head,
        *(
            pltpu.with_memory_space_constraint(x, pltpu.HBM)
            for x in (prefix_keys, prefix_values, suffix_keys, suffix_values)
        ),
    )


def attend_kernel(plan, place, pre_row, suf_row, lengths, query_ref, *refs):
    slots, ways, prefix_count, rows, shares, heads, first, last = plan
    refs = list(refs)
    block_refs = [(refs.pop(0), head_offset) for slot, head_offset in slots]
    slots = [slot for slot, head_offset in slots]
    prefix_refs = [(refs.pop(0), refs.pop(0)) for way in ways]
    state_ref = None if first else refs.pop(0)
    if last and heads[0] > 0:
        refs.pop(0)
    out_ref = refs.pop(0)
    if not last:
        state_ref = out_ref
    key_buffer, value_buffer, seen_list, out_buffer, out_semaphores = refs
    turns = heads[1] // TOGETHER
    per_share = KV_HEADS // shares
    seq_index, samp_index = place[0], place[1]
    row, column = seq_index // COLUMNS, seq_index % COLUMNS
    live = seq_index < lengths[0]

    def leave(turn):
        lanes = pl.ds((heads[0] + turn * TOGETHER) * WIDE, TOGETHER * WIDE)
        return pltpu.make_async_copy(
            out_buffer.at[turn], out_ref.at[:, lanes], out_semaphores.at[turn]
        )

    def suffix_seen(slot):
        back, across = slot
        side = 1 - column if across else column
        block = (row - back) * COLUMNS + side
        inside = (block >= 0) & (block < seq_index)
        return inside & (suf_row[jnp.maximum(block, 0)] > 0)

    def prefix_seen(n):
        side = jnp.where(n >= rows, 1 - column, column)
        back = n % rows
        block = jnp.where(row >= back, row - back, row - back + rows) * COLUMNS + side
        return pre_row[block] > 0

    @pl.when(live)
    def compute():
        places, suffix_end = [], jnp.int32(0)
        for slot in slots:
            seen = True if slot == (0, False) else suffix_seen(slot)
            places.append((seen, suffix_end))
            suffix_end = suffix_end + (1 if seen is True else seen.astype(jnp.int32))
        near_count = prefix_seen_count = jnp.int32(0)
        if prefix_count:

            def note(n, found):
                seen_list[found] = n
                return found + prefix_seen(n).astype(jnp.int32)

            near_count = lax.fori_loop(0, rows, note, jnp.int32(0))
            prefix_seen_count = lax.fori_loop(rows, prefix_count, note, near_count)

        def some_heads(turn, unused):
            head = heads[0] + turn * TOGETHER
            relative = (head // per_share) ^ samp_index
            my_way = relative % 2 * 2 + relative // 2
            lanes = range(TOGETHER)
            has_prefix = sum((my_way == way).astype(jnp.int32) for way in ways)
            count = suffix_end + prefix_seen_count * has_prefix

            def take(position, sources):
                for i, source in enumerate(sources):
                    key_buffer[i, position] = source[0]
                    value_buffer[i, position] = source[1]

            def take_block(n, position):
                ref, head_offset = block_refs[n]
                take(position, [ref.at[head - head_offset + i] for i in lanes])

            for n, (seen, position) in enumerate(places):
                if seen is True:
                    take_block(n, position)
                else:
                    pl.when(seen)(functools.partial(take_block, n, position))

            for way, pieces in zip(ways, prefix_refs):

                def take_prefix(ref, skipped, n, unused):
                    chosen = ref.at[seen_list[n] - skipped]
                    first_head = head % per_share
                    take(suffix_end + n, [chosen.at[first_head + i] for i in lanes])
                    return unused

                @pl.when(my_way == way)
                def _(pieces=pieces):
                    lax.fori_loop(0, near_count, functools.partial(take_prefix, pieces[0], 0), 0)
                    lax.fori_loop(
                        near_count,
                        prefix_seen_count,
                        functools.partial(take_prefix, pieces[1], rows),
                        0,
                    )

            offset = pl.multiple_of(head * WIDE, WIDE)
            wide = query_ref[:, pl.ds(offset, TOGETHER * WIDE)]
            queries = [
                jnp.concatenate(
                    [
                        wide[:, (i * GROUP + j) * HEAD_DIM : (i * GROUP + j + 1) * HEAD_DIM]
                        for j in range(GROUP)
                    ],
                    axis=0,
                )
                for i in lanes
            ]
            state = [state_ref.at[head + i] for i in lanes]
            sums = slice(HEAD_DIM + 8, HEAD_DIM + 16)

            def chunk(start, size, fresh):
                keys = [
                    key_buffer[i, pl.ds(start, size)].reshape(size * BLOCK, HEAD_DIM)
                    for i in lanes
                ]
                values = [
                    jnp.concatenate([value_buffer[i, start + n] for n in range(size)], axis=1)
                    for i in lanes
                ]
                before = [None if fresh else state[i][HEAD_DIM:] for i in lanes]
                tall = size * BLOCK // 8
                after = []
                for i in lanes:
                    scores = lax.dot_general(
                        keys[i],
                        queries[i],
                        (((1,), (1,)), ((), ())),
                        preferred_element_type=jnp.float32,
                    )
                    if fresh:
                        key_at = lax.broadcasted_iota(jnp.int32, (BLOCK, WIDE), 0)
                        query_at = lax.broadcasted_iota(jnp.int32, (BLOCK, WIDE), 1) % BLOCK
                        scores = jnp.where(key_at <= query_at, scores, masked_value)
                    new = jnp.max(scores, axis=0, keepdims=True)
                    if not fresh:
                        new = jnp.maximum(before[i][0:1], new)
                    weights = jnp.exp2((scores - new) * exponent_scale)
                    part_sum = jnp.sum(weights.reshape(tall, 8, WIDE), axis=0)
                    part = lax.dot_general(
                        values[i],
                        weights.astype(jnp.bfloat16),
                        (((1,), (0,)), ((), ())),
                        preferred_element_type=jnp.float32,
                    )
                    after.append((new, part_sum, part))
                for i in lanes:
                    new, part_sum, part = after[i]
                    if not fresh:
                        shrink = jnp.exp2((before[i][0:1] - new) * exponent_scale)
                        part_sum = part_sum + before[i][8:] * shrink
                        part = part + state[i][:HEAD_DIM] * shrink
                    state[i][:HEAD_DIM] = part
                    state[i][HEAD_DIM : HEAD_DIM + 8] = jnp.broadcast_to(new, (8, WIDE))
                    state[i][sums] = part_sum

            start = 0
            if first:
                chunk(0, 1, True)
                start = 1
            rest = count - start

            def many(n, unused):
                chunk(start + n * CHUNK, CHUNK, False)
                return unused

            largest = len(slots) + prefix_count - start
            if largest >= CHUNK:
                lax.fori_loop(0, rest // CHUNK, many, 0)
            size = CHUNK // 2
            while size:
                if largest >= size:

                    @pl.when(rest // size % 2 == 1)
                    def _(size=size):
                        chunk(start + rest // (2 * size) * (2 * size), size, False)

                size //= 2

            if last:
                parts = []
                for i in lanes:
                    inverse = 1.0 / jnp.sum(state[i][sums], axis=0, keepdims=True)
                    mixed = (state[i][:HEAD_DIM] * inverse).astype(jnp.bfloat16)
                    parts += [mixed[:, j * BLOCK : (j + 1) * BLOCK].T for j in range(GROUP)]
                out_buffer[turn] = jnp.concatenate(parts, axis=1)
                leave(turn).start()
            return unused

        lax.fori_loop(0, turns, some_heads, 0)

    if last:

        @pl.when(jnp.logical_not(live))
        def blank():
            out_buffer[...] = jnp.zeros_like(out_buffer)
            for turn in range(turns):
                leave(turn).start()

        for turn in range(turns):
            leave(turn).wait()


def attend(tables, queries, slots, blocks, prefix, state, out, heads, shares, rows):
    ways = tuple(prefix)
    prefix = [piece for way in ways for piece in prefix[way]]
    prefix_count = prefix[0].shape[0] * COLUMNS if prefix else 0
    first = state is None
    last = heads != (0, KV_HEADS)
    total = len(slots) + prefix_count
    plan = tuple((slot, head_offset) for slot, (block, head_offset) in zip(slots, blocks))
    inside = pl.BlockSpec(memory_space=pltpu.VMEM)
    outside = pl.BlockSpec(memory_space=pltpu.HBM)
    table = pl.BlockSpec(memory_space=pltpu.SMEM)
    operands = [queries, *(block for block, head_offset in blocks), *prefix]
    operands += [] if first else [state]
    operands = [pltpu.with_memory_space_constraint(x, pltpu.VMEM) for x in operands]
    in_specs = [table] * len(tables) + [inside] * len(operands)
    if last:
        out_shape = pltpu.HBM((BLOCK, HEADS * HEAD_DIM), jnp.bfloat16)
        if out is not None:
            operands.append(pltpu.with_memory_space_constraint(out, pltpu.HBM))
            in_specs.append(outside)
    else:
        out_shape = pltpu.VMEM((KV_HEADS, HEAD_DIM + 16, WIDE), jnp.float32)
    aliased = out is not None or not (first or last)
    turns = heads[1] // TOGETHER if last else 1
    buffer_width = TOGETHER * WIDE if last else HEAD_DIM
    return pl.pallas_call(
        functools.partial(
            attend_kernel, (plan, ways, prefix_count, rows, shares, heads, first, last)
        ),
        out_shape=out_shape,
        in_specs=in_specs,
        out_specs=outside if last else inside,
        scratch_shapes=[
            pltpu.VMEM((TOGETHER, total, BLOCK, HEAD_DIM), jnp.bfloat16),
            pltpu.VMEM((TOGETHER, total, HEAD_DIM, BLOCK), jnp.bfloat16),
            pltpu.SMEM((max(prefix_count, 1) + 1,), jnp.int32),
            pltpu.VMEM((turns, BLOCK, buffer_width), jnp.bfloat16),
            pltpu.SemaphoreType.DMA((turns,)),
        ],
        input_output_aliases={len(in_specs) - 1: 0} if aliased else {},
        compiler_params=pltpu.CompilerParams(vmem_limit_bytes=10 * 2**20 + total * 2**17),
    )(*tables, *operands)


def shards(
    queries, prefix_keys, prefix_values, suffix_keys, suffix_values, layout_pre, layout_suf, lengths
):
    seq_count = lax.axis_size("seq")
    shares = lax.axis_size("samp")
    rows = seq_count // COLUMNS
    seq_index = lax.axis_index("seq")
    samp_index = lax.axis_index("samp")
    per_share = KV_HEADS // shares

    def along_rows(pairs):
        return [(a * COLUMNS + y, b * COLUMNS + y) for a, b in pairs for y in range(COLUMNS)]

    def move(value, pairs, axis="seq"):
        return lax.ppermute(value, axis, pairs)

    swap_columns = [(i, i ^ 1) for i in range(seq_count)]
    first_head = (samp_index * per_share).astype(jnp.int32)
    own, own_share = pack(
        suffix_keys[0], suffix_values[0], prefix_keys, prefix_values, first_head[None], per_share
    )

    held = {(0, False): own}
    top = rows - 1
    low, high = slice(0, KV_HEADS // 2), slice(KV_HEADS // 2, KV_HEADS)
    across = [(z * COLUMNS, z * COLUMNS + 1) for z in range(rows)]
    held[0, True] = move(own, across)
    for k in range(1, rows):
        upward = along_rows([(z, z + 1) for z in range(k - 1, top)])
        if k < top or top == 1:
            held[k, False] = move(held[k - 1, False], upward)
            held[k, True] = move(held[k, False], swap_columns[k * COLUMNS :])
        else:
            from_row = along_rows([(1, top)])
            straight = move(held[1, False][low], from_row)
            relayed = move(held[k - 1, False][high], along_rows([(top - 1, top)]))
            held[k, False] = (straight, relayed)
            held[k, True] = tuple(move(held[1, True][part], from_row) for part in (low, high))

    gathered = [own_share]
    for k in range(1, rows):
        turn = along_rows([(z, (z + k) % rows) for z in range(rows)])
        gathered.append(move(own_share, turn))
    swap_x = [(i, i ^ 2) for i in range(shares)]
    swap_core = [(i, i ^ 1) for i in range(shares)]
    same = jnp.stack(gathered)
    other = move(same, swap_columns)
    same_x = move(same, swap_x, "samp")
    other_x = move(other, swap_x, "samp")
    near = [same, other, same_x, other_x]
    far = [move(piece, swap_core, "samp") for piece in near]
    straight_ways = {0: near[:2], 2: far[:2]}
    crossed_ways = {1: near[2:], 3: far[2:]}

    groups = stages(rows)
    groups[2] = [slot for slot in held if slot not in sum(groups, [])]
    tables = (
        jnp.stack([seq_index, samp_index]).astype(jnp.int32),
        layout_pre[0, 0],
        layout_suf[0, 0],
        lengths,
    )

    def run(slots, prefix, state, out, heads):
        blocks = []
        for slot in slots:
            split = isinstance(held[slot], tuple)
            blocks.append((held[slot][heads[0] > 0], heads[0]) if split else (held[slot], 0))
        return attend(tables, queries[0], slots, blocks, prefix, state, out, heads, shares, rows)

    state = None
    for n, prefix in enumerate([{}, straight_ways, crossed_ways]):
        state = run(groups[n], prefix, state, None, (0, KV_HEADS))
    half = KV_HEADS // 2
    out = run(groups[3], {}, state, None, (0, half))
    return run(groups[3], {}, state, out, (half, half))[None]


def stages(rows):
    return [
        [(0, False), (0, True)],
        [(1, False)],
        [],
        [(rows - 2, True), (rows - 1, False), (rows - 1, True)],
    ]


def solution(mesh):
    return jax.shard_map(
        shards,
        mesh=mesh,
        in_specs=(
            P("samp", "seq", None),
            P("seq", None),
            P("seq", None),
            P("samp", "seq", None),
            P("samp", "seq", None),
            P("samp", "seq", None),
            P("samp", "seq", None),
            P("samp"),
        ),
        out_specs=P("samp", "seq", None),
        check_vma=False,
    )
```
